32 devices in a mesh: cfg: 2 (over x), ta: 16 (over z, y, core).
Axes of the slice: x: 2, y: 2, z: 4, core: 2. Of those that a mesh axis runs over, the one named last changes fastest.
Arguments:
- fine_source: bfloat16 [32, 128, 2, 2, 24, 128], P('cfg', 'ta'), parts along dimension 0, may hold values from -24 to 24
- projectors: bfloat16 [32, 128, 2304], P(('cfg', 'ta')), parts along dimension 0, may hold values from -0.21875 to 0.21875
- stencil_links: bfloat16 [32, 8, 48, 864], P(('cfg', 'ta')), parts along dimension 0, may hold values from -0.21875 to 0.21875
- quark_mass: float32 [2], P('cfg'), parts along dimension 0, may hold values from 1.5 to 3
Outputs:
- solution: float32 [32, 8, 96, 128], P(('cfg', 'ta')), parts along dimension 0
- residual: float32 [32, 8, 96, 128], P(('cfg', 'ta')), parts along dimension 0
The draws below stay inside these ranges and needn't reach their ends.
There are 2 independent parts, one for each index of `cfg`. The reference program is written for one: setup_inputs(seed, part) draws one part's arguments, and reference() takes and returns one part's arrays. A program takes and returns all parts, laid end to end along the dimension named above; each array names one. Nothing has to cross between parts.
All inputs are finite; a program needn't handle non-finite values.
Results may differ from the reference program's by a relative error of at most 0.012.
The reference program's roundings to bfloat16 on the way count: a program that leaves them out, or rounds other values in their place, can miss the bound.
Values may be sent and summed in bfloat16 or wider, within the bound.
A program may use at most 128 MiB of HBM per device.

```python
import math
import jax
import jax.numpy as jnp
from jax import lax

NV = 24
LX = 4
LY = 2
LZ = 8
YX = 16
RHS = 128
ITERS = 3
CC = 48
LT = 2
PLANES = 16
XY = 8
COLS = 128
FK = 24


def draw_fine_source(key, part):
    shape_full = (PLANES, COLS, 2, 2, FK, RHS)
    key_base = jax.random.fold_in(key, 11)
    first_key = jax.random.fold_in(key_base, 0)
    third_key = jax.random.fold_in(key_base, 2)
    slices = (jnp.arange(PLANES) // LZ).astype(jnp.float32) / max(LT - 1, 1)
    values = jax.random.truncated_normal(first_key, -4.0, 4.0, shape_full)
    scales = jnp.exp(jax.random.uniform(third_key, (PLANES, COLS, 1, 1, 1, 1), minval=math.log(0.25), maxval=math.log(2.5)))
    time_ramp = jnp.exp(math.log(3.0) * slices - 0.5 * math.log(3.0))
    return (values * scales * time_ramp.reshape(PLANES, 1, 1, 1, 1, 1)).astype(jnp.bfloat16)


def steps_of(rng, extent, cuts, low, high):
    loudness, own = 1.0, jax.random.fold_in(rng, 6)
    for axis_at, parts in cuts:
        heights = jnp.exp(jax.random.uniform(jax.random.fold_in(own, axis_at), (parts,), jnp.float32, low / len(cuts), high / len(cuts)))
        loudness = loudness * jnp.repeat(heights, extent[axis_at] // parts).reshape([-1 if axis == axis_at else 1 for axis in range(len(extent))])
    return loudness


def normal_values(own_key, extent, spread, most, pieces=(), held_as=jnp.bfloat16):
    gain = steps_of(own_key, extent, pieces, -0.22, 0.18) if pieces else 1.0
    array = jax.random.normal(own_key, extent, jnp.float32) * spread * gain
    return jnp.minimum(jnp.maximum(array, -most), most).astype(held_as)


def setup_inputs(seed: int = 0, part: int = 0) -> dict:
    key_of = jax.random.split(jax.random.key(seed), 5)
    part_splits = jax.random.split(jax.random.fold_in(key_of[4], part), 5)
    return {
        "fine_source": draw_fine_source(jax.random.fold_in(jax.random.fold_in(key_of[4], part), 71), part),
        "projectors": normal_values(part_splits[1], (PLANES, COLS, 4 * NV * FK), (2 * YX * FK) ** -0.5, 0.21875, ((0, 16),)),
        "stencil_links": normal_values(part_splits[2], (PLANES, XY, CC, 18 * CC), (18 * CC) ** -0.5, 0.21875, ((0, 16),)),
        "quark_mass": jnp.clip(jax.random.uniform(part_splits[3], (1,), jnp.float32, 1.5, 3.0), 1.5, 3.0),
    }


roll_table = ((0, 0), (3, -1), (3, 1), (2, -1), (2, 1), (1, -1), (1, 1), (0, -1), (0, 1))

def restrict_plane(operands):
    fine_plane, proj_plane = operands
    fine_plane = fine_plane.astype(jnp.float32).reshape(XY, YX, 2, 2, FK, RHS)
    proj_plane = proj_plane.astype(jnp.float32).reshape(XY, YX, 2, NV, 2, FK)
    proj_re = proj_plane[:, :, :, :, 0, :]
    proj_im = proj_plane[:, :, :, :, 1, :]
    fine_re = fine_plane[:, :, 0]
    fine_im = fine_plane[:, :, 1]
    highest = lax.Precision.HIGHEST
    result_re = jnp.einsum('sohvk,sohkr->shvr', proj_re, fine_re, precision=highest) + jnp.einsum('sohvk,sohkr->shvr', proj_im, fine_im, precision=highest)
    result_im = jnp.einsum('sohvk,sohkr->shvr', proj_re, fine_im, precision=highest) - jnp.einsum('sohvk,sohkr->shvr', proj_im, fine_re, precision=highest)
    return jnp.stack([result_re, result_im], axis=1).reshape(XY, 2 * CC, RHS)

def apply_operator(vector, stencil_links, quark_mass):
    highest = lax.Precision.HIGHEST
    rounded = lax.optimization_barrier(vector.astype(jnp.bfloat16)).astype(jnp.float32)
    lattice = rounded.reshape(LT, LZ, LY, LX, 2 * CC, RHS)
    link_view = stencil_links.reshape(PLANES, XY, CC, 9, 2, CC)
    total_re = quark_mass[0] * rounded[:, :, :CC]
    total_im = quark_mass[0] * rounded[:, :, CC:]
    for direction in range(9):
        axis_number, offset = roll_table[direction]
        if direction == 0:
            neighbour = lattice
        else:
            neighbour = jnp.roll(lattice, offset, axis=axis_number)
        neighbour = neighbour.reshape(PLANES, XY, 2 * CC, RHS)
        near_re = neighbour[:, :, :CC]
        near_im = neighbour[:, :, CC:]
        link_re = link_view[:, :, :, direction, 0, :].astype(jnp.float32)
        link_im = link_view[:, :, :, direction, 1, :].astype(jnp.float32)
        total_re = total_re + jnp.einsum('psij,psjr->psir', link_re, near_re, precision=highest) - jnp.einsum('psij,psjr->psir', link_im, near_im, precision=highest)
        total_im = total_im + jnp.einsum('psij,psjr->psir', link_re, near_im, precision=highest) + jnp.einsum('psij,psjr->psir', link_im, near_re, precision=highest)
    return jnp.concatenate([total_re, total_im], axis=2)

def inner_product(left, right):
    left_re = left[:, :, :CC]
    left_im = left[:, :, CC:]
    right_re = right[:, :, :CC]
    right_im = right[:, :, CC:]
    return (lax.optimization_barrier(jnp.sum(left_re * right_re + left_im * right_im, axis=(0, 1, 2))), lax.optimization_barrier(jnp.sum(left_re * right_im - left_im * right_re, axis=(0, 1, 2))))

def scaled(vector, factor_re, factor_im):
    vector_re = vector[..., :CC, :]
    vector_im = vector[..., CC:, :]
    return jnp.concatenate([factor_re * vector_re - factor_im * vector_im, factor_re * vector_im + factor_im * vector_re], axis=-2)

def reference(fine_source, projectors, stencil_links, quark_mass):
    source = lax.map(restrict_plane, (fine_source, projectors))
    solution = jnp.zeros_like(source)
    residual = source
    basis_q = []
    basis_p = []
    for iteration in range(ITERS):
        direction = residual
        mapped = apply_operator(residual, stencil_links, quark_mass)
        coeffs = [inner_product(earlier, mapped) for earlier in basis_q]
        for number in range(iteration):
            mapped = mapped - scaled(basis_q[number], coeffs[number][0], coeffs[number][1])
            direction = direction - scaled(basis_p[number], coeffs[number][0], coeffs[number][1])
        squared = inner_product(mapped, mapped)[0]
        factor = 1.0 / jnp.sqrt(squared + 1e-06)
        unit_q = mapped * factor
        unit_p = direction * factor
        alpha_re, alpha_im = inner_product(unit_q, residual)
        solution = solution + scaled(unit_p, alpha_re, alpha_im)
        residual = residual - scaled(unit_q, alpha_re, alpha_im)
        basis_q.append(unit_q)
        basis_p.append(unit_p)
    return (solution, residual)
```

```python
import functools
import math

import jax
import jax.numpy as jnp
from jax import lax
from jax.experimental import pallas as pl
from jax.experimental.pallas import tpu as pltpu
from jax.sharding import PartitionSpec as P

LX = 4
LZ = 8
ITERS = 3


def from_behind(value, axis, steps):
    count = lax.axis_size(axis)
    pairs = [(source, (source + steps) % count) for source in range(count)]
    return lax.ppermute(value, axis, pairs)


def real_weights(proj_view):
    proj_re = proj_view[..., 0, :]
    proj_im = proj_view[..., 1, :]
    first_row = jnp.stack([proj_re, proj_im], axis=-4)
    second_row = jnp.stack([-proj_im, proj_re], axis=-4)
    return jnp.stack([first_row, second_row], axis=-5)


def inner_local(left, right, comp_count):
    left_re = left[:, :comp_count]
    left_im = left[:, comp_count:]
    right_re = right[:, :comp_count]
    right_im = right[:, comp_count:]
    return (
        jnp.sum(left_re * right_re + left_im * right_im, axis=(0, 1)),
        jnp.sum(left_re * right_im - left_im * right_re, axis=(0, 1)),
    )


def scaled(vector, factor_re, factor_im, comp_count):
    vector_re = vector[:, :comp_count]
    vector_im = vector[:, comp_count:]
    return jnp.concatenate(
        [
            factor_re * vector_re - factor_im * vector_im,
            factor_re * vector_im + factor_im * vector_re,
        ],
        axis=1,
    )


def shards_general(fine_source, projectors, stencil_links, quark_mass):
    comp_count = stencil_links.shape[2]
    null_count = comp_count // 2
    site_count = stencil_links.shape[1]
    column_count = projectors.shape[1]
    block_count = column_count // site_count
    fine_count = fine_source.shape[4]
    rhs_count = fine_source.shape[5]
    plane_count = fine_source.shape[0]
    moved_proj = lax.all_to_all(projectors, "ta", split_axis=1, concat_axis=0, tiled=True)
    local_columns = fine_source.shape[1]
    group_size = math.gcd(block_count, local_columns)
    groups = local_columns // group_size
    weights = real_weights(
        moved_proj.reshape(plane_count, groups, group_size, 2, null_count, 2, fine_count)
    )
    fine_local = fine_source.reshape(plane_count, groups, group_size, 2, 2, fine_count, rhs_count)
    partial_sums = jnp.einsum(
        "pmgdchvk,pmgchkr->pmdhvr", weights, fine_local, preferred_element_type=jnp.float32
    )
    partial_sums = partial_sums.reshape(plane_count, groups, 2 * comp_count, rhs_count)
    collected = lax.all_to_all(partial_sums, "ta", split_axis=0, concat_axis=1, tiled=True)
    source = jnp.sum(
        collected.reshape(site_count, block_count // group_size, 2 * comp_count, rhs_count), axis=1
    )
    link_view = stencil_links.reshape(site_count, comp_count, 9, 2, comp_count)
    link_re = link_view[:, :, :, 0, :]
    link_im = link_view[:, :, :, 1, :]
    upper_rows = jnp.stack([link_re, -link_im], axis=3)
    lower_rows = jnp.stack([link_im, link_re], axis=3)
    real_operator = jnp.stack([upper_rows, lower_rows], axis=1).reshape(
        site_count, 2 * comp_count, 18 * comp_count
    )
    mass_value = quark_mass[0]
    z_position = lax.axis_index("ta") % LZ
    line_count = site_count // LX

    def flatten_sites(shifted):
        return shifted.reshape(site_count, 2 * comp_count, rhs_count)

    solution = jnp.zeros_like(source)
    residual = source
    basis_q = []
    basis_p = []
    for iteration in range(ITERS):
        direction = residual
        rounded = residual.astype(jnp.bfloat16)
        plane_view = rounded.reshape(line_count, LX, 2 * comp_count, rhs_count)
        x_plus = flatten_sites(jnp.roll(plane_view, -1, axis=1))
        x_minus = flatten_sites(jnp.roll(plane_view, 1, axis=1))
        y_plus = flatten_sites(jnp.roll(plane_view, -1, axis=0))
        y_minus = flatten_sites(jnp.roll(plane_view, 1, axis=0))
        z_plus_near = from_behind(rounded, "ta", -1)
        z_minus_near = from_behind(rounded, "ta", 1)
        upper_pair = from_behind(jnp.stack([rounded, z_minus_near], axis=0), "ta", -LZ)
        lower_pair = from_behind(jnp.stack([rounded, z_plus_near], axis=0), "ta", LZ)
        t_plus = upper_pair[0]
        t_minus = lower_pair[0]
        z_plus = jnp.where(z_position == LZ - 1, lower_pair[1], z_plus_near)
        z_minus = jnp.where(z_position == 0, upper_pair[1], z_minus_near)
        stacked = jnp.stack(
            [rounded, x_plus, x_minus, y_plus, y_minus, z_plus, z_minus, t_plus, t_minus], axis=1
        )
        stacked = stacked.reshape(site_count, 18 * comp_count, rhs_count)
        product = jnp.einsum(
            "sij,sjr->sir", real_operator, stacked, preferred_element_type=jnp.float32
        )
        mapped = product + mass_value * rounded.astype(jnp.float32)
        square_loc = inner_local(mapped, mapped, comp_count)[0]
        cross_re, cross_im = inner_local(mapped, residual, comp_count)
        if iteration > 0:
            coef_pairs = [inner_local(earlier, mapped, comp_count) for earlier in basis_q]
            back_pairs = [inner_local(earlier, residual, comp_count) for earlier in basis_q]
            coef_re = jnp.stack([pair[0] for pair in coef_pairs])
            coef_im = jnp.stack([pair[1] for pair in coef_pairs])
            back_re = jnp.stack([pair[0] for pair in back_pairs])
            back_im = jnp.stack([pair[1] for pair in back_pairs])
        else:
            coef_re = jnp.zeros((1, rhs_count), jnp.float32)
            coef_im = jnp.zeros((1, rhs_count), jnp.float32)
            back_re = jnp.zeros((1, rhs_count), jnp.float32)
            back_im = jnp.zeros((1, rhs_count), jnp.float32)
        square_all, cross_re, cross_im, coef_re, coef_im, back_re, back_im = lax.psum(
            (square_loc, cross_re, cross_im, coef_re, coef_im, back_re, back_im), "ta"
        )
        squared = square_all
        proj_re = cross_re
        proj_im = cross_im
        for number in range(iteration):
            mapped = mapped - scaled(basis_q[number], coef_re[number], coef_im[number], comp_count)
            direction = direction - scaled(
                basis_p[number], coef_re[number], coef_im[number], comp_count
            )
            squared = squared - (
                coef_re[number] * coef_re[number] + coef_im[number] * coef_im[number]
            )
            proj_re = proj_re - (
                coef_re[number] * back_re[number] + coef_im[number] * back_im[number]
            )
            proj_im = proj_im - (
                coef_re[number] * back_im[number] - coef_im[number] * back_re[number]
            )
        factor = 1.0 / jnp.sqrt(squared + 1e-06)
        unit_q = mapped * factor
        unit_p = direction * factor
        alpha_re = proj_re * factor
        alpha_im = proj_im * factor
        solution = solution + scaled(unit_p, alpha_re, alpha_im, comp_count)
        residual = residual - scaled(unit_q, alpha_re, alpha_im, comp_count)
        basis_q.append(unit_q)
        basis_p.append(unit_p)
    return (
        solution.reshape(1, site_count, 2 * comp_count, rhs_count),
        residual.reshape(1, site_count, 2 * comp_count, rhs_count),
    )


MESH = pl.DeviceIdType.MESH


def flipped(number, mask, bits):
    total = 0
    for bit in range(bits):
        size = 1 << bit
        total = total + (((number // size) % 2 + (mask // size) % 2) % 2) * size
    return total


def widened(plane):
    half = plane.shape[0] // 2
    real, imag = plane[:half], plane[half:]
    return jnp.concatenate(
        [jnp.concatenate([real, imag], axis=1), jnp.concatenate([-imag, real], axis=1)], axis=0
    )


def solve_kernel(
    count, sites, comps,
    mass_ref, weights_ref, fine_hbm, links_hbm,
    sol_ref, res_ref,
    fine_ref, links_ref, near_ref, zlinks_ref, tlinks_ref, mask_ref,
    weights_in, part_keep, part_out, part_in, sum_out, source_ref,
    wide_ref, round_ref, halo_ref, acc_ref, basis_q, basis_p, stat_out, stat_in,
    local_sem, wsend, wrecv, psend, precv, ssend, srecv, hsend, hrecv, gsend, grecv,
):
    me = lax.axis_index("ta")
    bits = count.bit_length() - 1
    core = me % 2
    chip = me // 2
    partner = chip * 2 + 1 - core
    chips = count // 2
    null = comps // 2
    rows = fine_ref.shape[1]
    rhs = fine_ref.shape[2]

    fine_copy = pltpu.make_async_copy(fine_hbm, fine_ref, local_sem.at[0])
    fine_copy.start()
    links_copy = pltpu.make_async_copy(links_hbm, links_ref, local_sem.at[1])
    links_copy.start()

    barrier = pltpu.get_barrier_semaphore()

    def greet(step, carry):
        pl.semaphore_signal(
            barrier, inc=1, device_id={"ta": flipped(me, step, bits)}, device_id_type=MESH
        )
        return carry

    lax.fori_loop(1, count, greet, 0)
    pl.semaphore_wait(barrier, count - 1)

    def weights_copy(slot, other, origin):
        return pltpu.make_async_remote_copy(
            src_ref=weights_ref.at[slot], dst_ref=weights_in.at[origin],
            send_sem=wsend.at[slot], recv_sem=wrecv.at[origin],
            device_id={"ta": other}, device_id_type=MESH,
        )

    def send_weights(step, carry):
        other = flipped(me, count - 1 - step, bits)
        weights_copy(other, other, me).start()
        return carry

    lax.fori_loop(0, count - 1, send_weights, 0)

    rows_at = lax.broadcasted_iota(jnp.int32, (rows, rhs), 0)
    mask_ref[...] = (1 - (rows_at // null) % 2).astype(jnp.float32).astype(jnp.bfloat16)
    links_copy.wait()
    for site in range(sites):
        near_ref[site] = links_ref[site, :, : 10 * comps]
        zlinks_ref[site] = links_ref[site, :, 10 * comps : 14 * comps]
        tlinks_ref[site] = links_ref[site, :, 14 * comps : 18 * comps]
    fine_copy.wait()

    def restricted(plane, weights):
        fine = fine_ref[plane]
        first = fine * mask_ref[...]
        second = fine - first

        def turned(value):
            view = value.reshape(rows // (2 * comps), 2, comps, rhs)
            return jnp.stack([view[:, 1], -view[:, 0]], axis=1).reshape(rows, rhs)

        right = jnp.concatenate([first, second, turned(first), turned(second)], axis=1)
        half = rows // 2
        upper = jnp.dot(weights, right[:half], preferred_element_type=jnp.float32)
        lower = jnp.dot(weights, right[half:], preferred_element_type=jnp.float32)
        total = upper[:null] + lower[null:]
        return jnp.concatenate([total[:, k * rhs : (k + 1) * rhs] for k in range(4)], axis=0)

    def part_copy(slot):
        return pltpu.make_async_remote_copy(
            src_ref=part_out.at[slot], dst_ref=part_in.at[slot],
            send_sem=psend.at[slot], recv_sem=precv.at[slot],
            device_id={"ta": partner}, device_id_type=MESH,
        )

    def source_copy(slot, origin):
        return pltpu.make_async_remote_copy(
            src_ref=sum_out.at[slot], dst_ref=source_ref.at[origin],
            send_sem=ssend.at[slot], recv_sem=srecv.at[origin],
            device_id={"ta": flipped(chip, slot, bits - 1) * 2 + core}, device_id_type=MESH,
        )

    def pair(step):
        other = flipped(chip, step, bits - 1)
        away = other * 2 + 1 - core
        weights_copy(me, partner, away).wait_recv()
        part_out[step] = restricted(away, weights_in[away])
        part_copy(step).start()
        kept = other * 2 + core
        weights_copy(me, partner, kept).wait_recv()
        part_keep[step] = restricted(kept, weights_in[kept])

    def finish(step):
        part_copy(step).wait_recv()
        sum_out[step] = part_keep[step] + part_in[step]
        source_copy(step, chip).start()

    weights_copy(me, partner, partner).wait_recv()
    part_out[0] = restricted(partner, weights_in[partner])
    part_copy(0).start()
    part_keep[0] = restricted(me, weights_ref[me])
    pair(1)
    part_copy(0).wait_recv()
    source_ref[chip] = part_keep[0] + part_in[0]

    def pair_step(step, carry):
        pair(step)
        finish(step - 1)
        return carry

    lax.fori_loop(2, chips, pair_step, 0)
    finish(chips - 1)

    def source_wait(step, carry):
        source_copy(step, flipped(chip, step, bits - 1)).wait_recv()
        return carry

    lax.fori_loop(1, chips, source_wait, 0)

    mass = mass_ref[0]
    base = (me // LZ) * LZ
    z_at = me % LZ
    above = base + (z_at + 1) % LZ
    below = base + (z_at + LZ - 1) % LZ
    other_time = (me + LZ) % count
    targets = (other_time, above, below)
    lines = sites // LX

    def place(site, dx, dy):
        return ((site // LX + dy) % lines) * LX + (site % LX + dx) % LX

    def halo_copy(iteration, which):
        return pltpu.make_async_remote_copy(
            src_ref=round_ref.at[iteration], dst_ref=halo_ref.at[iteration, which],
            send_sem=hsend.at[iteration, which], recv_sem=hrecv.at[iteration, which],
            device_id={"ta": targets[which]}, device_id_type=MESH,
        )

    def stat_copy(iteration, other, origin):
        return pltpu.make_async_remote_copy(
            src_ref=stat_out.at[iteration], dst_ref=stat_in.at[iteration, origin],
            send_sem=gsend.at[iteration, other], recv_sem=grecv.at[iteration, origin],
            device_id={"ta": other}, device_id_type=MESH,
        )

    def times(factor, value):
        real, imag = value[:comps], value[comps:]
        return jnp.concatenate(
            [factor[0] * real - factor[1] * imag, factor[0] * imag + factor[1] * real], axis=0
        )

    factors, alphas, epsilons, overlap = [], [], [], None
    backs = []
    for it in range(ITERS):
        old = source_ref if it == 0 else res_ref
        for site in range(sites):
            round_ref[it, site] = old[site].astype(jnp.bfloat16)
        for which in range(3):
            halo_copy(it, which).start()
        for site in range(sites):
            wide_ref[site] = widened(round_ref[it, site])
        for site in range(sites):
            steps = ((0, 0), (1, 0), (-1, 0), (0, 1), (0, -1))
            right = jnp.concatenate([wide_ref[place(site, dx, dy)] for dx, dy in steps], axis=0)
            acc_ref[site] = jnp.dot(near_ref[site], right, preferred_element_type=jnp.float32)
        halo_copy(it, 2).wait_recv()
        halo_copy(it, 1).wait_recv()
        for site in range(sites):
            right = jnp.concatenate(
                [widened(halo_ref[it, 2, site]), widened(halo_ref[it, 1, site])], axis=0
            )
            acc_ref[site] += jnp.dot(zlinks_ref[site], right, preferred_element_type=jnp.float32)
        halo_copy(it, 0).wait_recv()
        sums = [0.0] * (3 + 2 * it)
        for site in range(sites):
            wide = widened(halo_ref[it, 0, site])
            right = jnp.concatenate([wide, wide], axis=0)
            product = acc_ref[site] + jnp.dot(
                tlinks_ref[site], right, preferred_element_type=jnp.float32
            )
            rounded = mass * round_ref[it, site].astype(jnp.float32)
            q_re = product[:, :rhs] + rounded[:comps]
            q_im = product[:, rhs:] + rounded[comps:]
            acc_ref[site] = jnp.concatenate([q_re, q_im], axis=1)
            r_re, r_im = old[site, :comps], old[site, comps:]
            sums[0] += q_re * q_re + q_im * q_im
            sums[1] += q_re * r_re + q_im * r_im
            sums[2] += q_re * r_im - q_im * r_re
            for j in range(it):
                b_re, b_im = basis_q[j, site, :comps], basis_q[j, site, comps:]
                sums[3 + 2 * j] += b_re * q_re + b_im * q_im
                sums[4 + 2 * j] += b_re * q_im - b_im * q_re
        lines_of = [jnp.sum(value, axis=0, keepdims=True) for value in sums]
        lines_of += [jnp.zeros((8 - len(lines_of), rhs), jnp.float32)]
        stats = jnp.concatenate(lines_of, axis=0)
        stat_out[it] = stats

        def send_stats(step, carry, it=it):
            other = flipped(me, count - 1 - step, bits)
            stat_copy(it, other, me).start()
            return carry

        lax.fori_loop(0, count - 1, send_stats, 0)
        stat_in[it, me] = stats

        def wait_stats(step, carry, it=it):
            other = flipped(me, step, bits)
            stat_copy(it, other, other).wait_recv()
            return carry

        lax.fori_loop(1, count, wait_stats, 0)
        total = jnp.sum(stat_in[it], axis=0)
        squared, cross_re, cross_im = total[0:1], total[1:2], total[2:3]
        coefs = [(total[3 + 2 * j : 4 + 2 * j], total[4 + 2 * j : 5 + 2 * j]) for j in range(it)]
        for j, (c_re, c_im) in enumerate(coefs):
            squared = squared - (c_re * c_re + c_im * c_im) * (1.0 + epsilons[j])
            cross_re = cross_re - (c_re * backs[j][0] + c_im * backs[j][1])
            cross_im = cross_im - (c_re * backs[j][1] - c_im * backs[j][0])
        if it == 2:
            (a_re, a_im), (b_re, b_im) = coefs
            pair_re, pair_im = a_re * b_re + a_im * b_im, a_re * b_im - a_im * b_re
            squared = squared + 2.0 * (pair_re * overlap[0] - pair_im * overlap[1])
        factor = 1.0 / jnp.sqrt(squared + 1e-06)
        alpha = (cross_re * factor, cross_im * factor)
        epsilon = 1e-06 * factor * factor
        if it == 1:
            overlap = (coefs[0][0] * epsilons[0] * factor, coefs[0][1] * epsilons[0] * factor)
            backs[0] = (
                backs[0][0] - (alpha[0] * overlap[0] - alpha[1] * overlap[1]),
                backs[0][1] - (alpha[0] * overlap[1] + alpha[1] * overlap[0]),
            )
        backs.append((alpha[0] * epsilon, alpha[1] * epsilon))
        epsilons.append(epsilon)
        for site in range(sites):
            residual = old[site]
            q = acc_ref[site]
            q = jnp.concatenate([q[:, :rhs], q[:, rhs:]], axis=0)
            p = residual
            for j in range(it):
                q = q - times(coefs[j], basis_q[j, site])
                p = p - times(coefs[j], basis_p[j, site])
            q = q * factor
            p = p * factor
            if it < ITERS - 1:
                basis_q[it, site] = q
                basis_p[it, site] = p
            step = times(alpha, p)
            sol_ref[site] = step if it == 0 else sol_ref[site] + step
            res_ref[site] = residual - times(alpha, q)

    def drain(step, carry):
        other = flipped(me, step, bits)
        weights_copy(other, other, me).wait_send()
        for it in range(ITERS):
            stat_copy(it, other, me).wait_send()
        return carry

    lax.fori_loop(1, count, drain, 0)
    part_copy(0).wait_send()

    def drain_parts(step, carry):
        part_copy(step).wait_send()
        source_copy(step, chip).wait_send()
        return carry

    lax.fori_loop(1, chips, drain_parts, 0)
    for it in range(ITERS):
        for which in range(3):
            halo_copy(it, which).wait_send()


def shards_kernel(fine_source, projectors, stencil_links, quark_mass):
    count = lax.axis_size("ta")
    planes, local_columns, _, _, null, rhs = fine_source.shape
    sites, comps = stencil_links.shape[1], stencil_links.shape[2]
    rows = local_columns * 4 * null
    fine = fine_source.reshape(planes, rows, rhs)
    weights = projectors.reshape(count, 2, local_columns // 2, 2, null, 2, null)
    weights = weights.transpose(0, 1, 4, 2, 5, 3, 6).reshape(count, 2 * null, rows // 2)
    links = stencil_links.reshape(sites, comps, 18 * comps)
    chips = count // 2
    vector = (sites, 2 * comps, rhs)
    f32, bf16 = jnp.float32, jnp.bfloat16
    dma = pltpu.SemaphoreType.DMA
    vmem = pl.BlockSpec(memory_space=pltpu.VMEM)
    hbm = pl.BlockSpec(memory_space=pl.ANY)
    parts = (chips, 2 * comps, rhs)
    sol, res = pl.pallas_call(
        functools.partial(solve_kernel, count, sites, comps),
        out_shape=[jax.ShapeDtypeStruct(vector, f32)] * 2,
        in_specs=[pl.BlockSpec(memory_space=pltpu.SMEM), vmem, hbm, hbm],
        out_specs=[vmem, vmem],
        scratch_shapes=[
            pltpu.VMEM(fine.shape, bf16),
            pltpu.VMEM(links.shape, bf16),
            pltpu.VMEM((sites, comps, 10 * comps), bf16),
            pltpu.VMEM((sites, comps, 4 * comps), bf16),
            pltpu.VMEM((sites, comps, 4 * comps), bf16),
            pltpu.VMEM((rows, rhs), bf16),
            pltpu.VMEM(weights.shape, bf16),
            pltpu.VMEM(parts, f32),
            pltpu.VMEM(parts, f32),
            pltpu.VMEM(parts, f32),
            pltpu.VMEM(parts, f32),
            pltpu.VMEM(vector, f32),
            pltpu.VMEM((sites, 2 * comps, 2 * rhs), bf16),
            pltpu.VMEM((ITERS, *vector), bf16),
            pltpu.VMEM((ITERS, 3, *vector), bf16),
            pltpu.VMEM((sites, comps, 2 * rhs), f32),
            pltpu.VMEM((ITERS - 1, *vector), f32),
            pltpu.VMEM((ITERS - 1, *vector), f32),
            pltpu.VMEM((ITERS, 8, rhs), f32),
            pltpu.VMEM((ITERS, count, 8, rhs), f32),
            dma((2,)),
            dma((count,)),
            dma((count,)),
            dma((chips,)),
            dma((chips,)),
            dma((chips,)),
            dma((chips,)),
            dma((ITERS, 3)),
            dma((ITERS, 3)),
            dma((ITERS, count)),
            dma((ITERS, count)),
        ],
        compiler_params=pltpu.CompilerParams(
            collective_id=0, has_side_effects=True, vmem_limit_bytes=60 * 1024 * 1024
        ),
    )(quark_mass, weights, fine, links)
    return sol.reshape(1, *vector), res.reshape(1, *vector)


def shards(fine_source, projectors, stencil_links, quark_mass):
    count = lax.axis_size("ta")
    sites = stencil_links.shape[1]
    local_columns = fine_source.shape[1]
    block = projectors.shape[1] // sites
    fits = (
        count == 2 * LZ
        and count == 2 * sites
        and count & (count - 1) == 0
        and block == 2 * local_columns
        and fine_source.shape[0] == count
        and ITERS == 3
    )
    chosen = shards_kernel if fits else shards_general
    return chosen(fine_source, projectors, stencil_links, quark_mass)


def solution(mesh):
    return jax.shard_map(
        shards,
        mesh=mesh,
        in_specs=(
            P("cfg", "ta", None, None, None, None),
            P(("cfg", "ta"), None, None),
            P(("cfg", "ta"), None, None, None),
            P("cfg"),
        ),
        out_specs=(P(("cfg", "ta"), None, None, None), P(("cfg", "ta"), None, None, None)),
        check_vma=False,
    )
```

```python
import functools
import math

import jax
import jax.numpy as jnp
from jax import lax
from jax.experimental import pallas as pl
from jax.experimental.pallas import tpu as pltpu
from jax.sharding import PartitionSpec as P

LX = 4
LZ = 8
ITERS = 3


def from_behind(value, axis, steps):
    count = lax.axis_size(axis)
    pairs = [(source, (source + steps) % count) for source in range(count)]
    return lax.ppermute(value, axis, pairs)


def real_weights(proj_view):
    proj_re = proj_view[..., 0, :]
    proj_im = proj_view[..., 1, :]
    first_row = jnp.stack([proj_re, proj_im], axis=-4)
    second_row = jnp.stack([-proj_im, proj_re], axis=-4)
    return jnp.stack([first_row, second_row], axis=-5)


def inner_local(left, right, comp_count):
    left_re = left[:, :comp_count]
    left_im = left[:, comp_count:]
    right_re = right[:, :comp_count]
    right_im = right[:, comp_count:]
    return (
        jnp.sum(left_re * right_re + left_im * right_im, axis=(0, 1)),
        jnp.sum(left_re * right_im - left_im * right_re, axis=(0, 1)),
    )


def scaled(vector, factor_re, factor_im, comp_count):
    vector_re = vector[:, :comp_count]
    vector_im = vector[:, comp_count:]
    return jnp.concatenate(
        [
            factor_re * vector_re - factor_im * vector_im,
            factor_re * vector_im + factor_im * vector_re,
        ],
        axis=1,
    )


def shards_general(fine_source, projectors, stencil_links, quark_mass):
    comp_count = stencil_links.shape[2]
    null_count = comp_count // 2
    site_count = stencil_links.shape[1]
    column_count = projectors.shape[1]
    block_count = column_count // site_count
    fine_count = fine_source.shape[4]
    rhs_count = fine_source.shape[5]
    plane_count = fine_source.shape[0]
    moved_proj = lax.all_to_all(projectors, "ta", split_axis=1, concat_axis=0, tiled=True)
    local_columns = fine_source.shape[1]
    group_size = math.gcd(block_count, local_columns)
    groups = local_columns // group_size
    weights = real_weights(
        moved_proj.reshape(plane_count, groups, group_size, 2, null_count, 2, fine_count)
    )
    fine_local = fine_source.reshape(plane_count, groups, group_size, 2, 2, fine_count, rhs_count)
    partial_sums = jnp.einsum(
        "pmgdchvk,pmgchkr->pmdhvr", weights, fine_local, preferred_element_type=jnp.float32
    )
    partial_sums = partial_sums.reshape(plane_count, groups, 2 * comp_count, rhs_count)
    collected = lax.all_to_all(partial_sums, "ta", split_axis=0, concat_axis=1, tiled=True)
    source = jnp.sum(
        collected.reshape(site_count, block_count // group_size, 2 * comp_count, rhs_count), axis=1
    )
    link_view = stencil_links.reshape(site_count, comp_count, 9, 2, comp_count)
    link_re = link_view[:, :, :, 0, :]
    link_im = link_view[:, :, :, 1, :]
    upper_rows = jnp.stack([link_re, -link_im], axis=3)
    lower_rows = jnp.stack([link_im, link_re], axis=3)
    real_operator = jnp.stack([upper_rows, lower_rows], axis=1).reshape(
        site_count, 2 * comp_count, 18 * comp_count
    )
    mass_value = quark_mass[0]
    z_position = lax.axis_index("ta") % LZ
    line_count = site_count // LX

    def flatten_sites(shifted):
        return shifted.reshape(site_count, 2 * comp_count, rhs_count)

    solution = jnp.zeros_like(source)
    residual = source
    basis_q = []
    basis_p = []
    for iteration in range(ITERS):
        direction = residual
        rounded = residual.astype(jnp.bfloat16)
        plane_view = rounded.reshape(line_count, LX, 2 * comp_count, rhs_count)
        x_plus = flatten_sites(jnp.roll(plane_view, -1, axis=1))
        x_minus = flatten_sites(jnp.roll(plane_view, 1, axis=1))
        y_plus = flatten_sites(jnp.roll(plane_view, -1, axis=0))
        y_minus = flatten_sites(jnp.roll(plane_view, 1, axis=0))
        z_plus_near = from_behind(rounded, "ta", -1)
        z_minus_near = from_behind(rounded, "ta", 1)
        upper_pair = from_behind(jnp.stack([rounded, z_minus_near], axis=0), "ta", -LZ)
        lower_pair = from_behind(jnp.stack([rounded, z_plus_near], axis=0), "ta", LZ)
        t_plus = upper_pair[0]
        t_minus = lower_pair[0]
        z_plus = jnp.where(z_position == LZ - 1, lower_pair[1], z_plus_near)
        z_minus = jnp.where(z_position == 0, upper_pair[1], z_minus_near)
        stacked = jnp.stack(
            [rounded, x_plus, x_minus, y_plus, y_minus, z_plus, z_minus, t_plus, t_minus], axis=1
        )
        stacked = stacked.reshape(site_count, 18 * comp_count, rhs_count)
        product = jnp.einsum(
            "sij,sjr->sir", real_operator, stacked, preferred_element_type=jnp.float32
        )
        mapped = product + mass_value * rounded.astype(jnp.float32)
        square_loc = inner_local(mapped, mapped, comp_count)[0]
        cross_re, cross_im = inner_local(mapped, residual, comp_count)
        if iteration > 0:
            coef_pairs = [inner_local(earlier, mapped, comp_count) for earlier in basis_q]
            back_pairs = [inner_local(earlier, residual, comp_count) for earlier in basis_q]
            coef_re = jnp.stack([pair[0] for pair in coef_pairs])
            coef_im = jnp.stack([pair[1] for pair in coef_pairs])
            back_re = jnp.stack([pair[0] for pair in back_pairs])
            back_im = jnp.stack([pair[1] for pair in back_pairs])
        else:
            coef_re = jnp.zeros((1, rhs_count), jnp.float32)
            coef_im = jnp.zeros((1, rhs_count), jnp.float32)
            back_re = jnp.zeros((1, rhs_count), jnp.float32)
            back_im = jnp.zeros((1, rhs_count), jnp.float32)
        square_all, cross_re, cross_im, coef_re, coef_im, back_re, back_im = lax.psum(
            (square_loc, cross_re, cross_im, coef_re, coef_im, back_re, back_im), "ta"
        )
        squared = square_all
        proj_re = cross_re
        proj_im = cross_im
        for number in range(iteration):
            mapped = mapped - scaled(basis_q[number], coef_re[number], coef_im[number], comp_count)
            direction = direction - scaled(
                basis_p[number], coef_re[number], coef_im[number], comp_count
            )
            squared = squared - (
                coef_re[number] * coef_re[number] + coef_im[number] * coef_im[number]
            )
            proj_re = proj_re - (
                coef_re[number] * back_re[number] + coef_im[number] * back_im[number]
            )
            proj_im = proj_im - (
                coef_re[number] * back_im[number] - coef_im[number] * back_re[number]
            )
        factor = 1.0 / jnp.sqrt(squared + 1e-06)
        unit_q = mapped * factor
        unit_p = direction * factor
        alpha_re = proj_re * factor
        alpha_im = proj_im * factor
        solution = solution + scaled(unit_p, alpha_re, alpha_im, comp_count)
        residual = residual - scaled(unit_q, alpha_re, alpha_im, comp_count)
        basis_q.append(unit_q)
        basis_p.append(unit_p)
    return (
        solution.reshape(1, site_count, 2 * comp_count, rhs_count),
        residual.reshape(1, site_count, 2 * comp_count, rhs_count),
    )


MESH = pl.DeviceIdType.MESH


def flipped(number, mask, bits):
    total = 0
    for bit in range(bits):
        size = 1 << bit
        total = total + (((number // size) % 2 + (mask // size) % 2) % 2) * size
    return total


def widened(plane):
    half = plane.shape[0] // 2
    real, imag = plane[:half], plane[half:]
    return jnp.concatenate(
        [jnp.concatenate([real, imag], axis=1), jnp.concatenate([-imag, real], axis=1)], axis=0
    )


def solve_kernel(
    count, sites, comps,
    mass_ref, proj_ref, fine_hbm, links_hbm,
    sol_ref, res_ref,
    fine_ref, links_ref, near_ref, zlinks_ref, tlinks_ref, fold_ref,
    weights_ref, weights_in, part_keep, part_out, part_in, sum_out, source_ref,
    wide_ref, round_ref, halo_ref, acc_ref, basis_q, basis_p, stat_out, stat_in,
    local_sem, wsend, wrecv, psend, precv, ssend, srecv, hsend, hrecv, gsend, grecv,
):
    me = lax.axis_index("ta")
    bits = count.bit_length() - 1
    core = me % 2
    chip = me // 2
    partner = chip * 2 + 1 - core
    chips = count // 2
    null = comps // 2
    rows = fine_ref.shape[1]
    rhs = fine_ref.shape[2]

    fine_copy = pltpu.make_async_copy(fine_hbm, fine_ref, local_sem.at[0])
    fine_copy.start()
    links_copy = pltpu.make_async_copy(links_hbm, links_ref, local_sem.at[1])
    links_copy.start()

    barrier = pltpu.get_barrier_semaphore()

    def greet(step, carry):
        pl.semaphore_signal(
            barrier, inc=1, device_id={"ta": flipped(me, step, bits)}, device_id_type=MESH
        )
        return carry

    lax.fori_loop(1, count, greet, 0)
    pl.semaphore_wait(barrier, count - 1)

    def weights_copy(slot, other, origin):
        return pltpu.make_async_remote_copy(
            src_ref=weights_ref.at[slot], dst_ref=weights_in.at[origin],
            send_sem=wsend.at[slot], recv_sem=wrecv.at[origin],
            device_id={"ta": other}, device_id_type=MESH,
        )

    columns = proj_ref.shape[1]
    width = columns * comps
    groups = comps // columns
    lane_at = lax.broadcasted_iota(jnp.int32, (columns, width), 1) // comps
    row_at = lax.broadcasted_iota(jnp.int32, (columns, width), 0)
    picks = (lane_at == row_at).astype(jnp.float32)
    fold_row = lax.broadcasted_iota(jnp.int32, (width, width), 0) % comps
    fold_lane = lax.broadcasted_iota(jnp.int32, (width, width), 1) % comps
    fold_ref[...] = (fold_row == fold_lane).astype(jnp.float32).astype(jnp.bfloat16)

    def arrange(slot):
        raw = proj_ref[slot].astype(jnp.float32)
        pieces = []
        for column in range(columns):
            for group in range(groups):
                row = raw[column : column + 1, group * width : (group + 1) * width]
                pieces.append(row * picks)
        left = jnp.concatenate(pieces, axis=0).astype(jnp.bfloat16)
        spread = jnp.dot(left, fold_ref[...], preferred_element_type=jnp.float32)
        total = spread[:comps] * picks[0:1]
        for column in range(1, columns):
            block = spread[column * comps : (column + 1) * comps]
            total = total + block * picks[column : column + 1]
        weights_ref[slot] = total.astype(jnp.bfloat16)

    def send_weights(step, carry):
        other = flipped(me, count - 1 - step, bits)
        arrange(other)
        weights_copy(other, other, me).start()
        return carry

    lax.fori_loop(0, count - 1, send_weights, 0)
    arrange(me)

    links_copy.wait()
    for site in range(sites):
        near_ref[site] = links_ref[site, :, : 10 * comps]
        zlinks_ref[site] = links_ref[site, :, 10 * comps : 14 * comps]
        tlinks_ref[site] = links_ref[site, :, 14 * comps : 18 * comps]
    fine_copy.wait()

    def restricted(plane, weights):
        fine = fine_ref[plane].astype(jnp.float32).reshape(columns, 2, 2, null, rhs)

        def ordered(real, imag, half):
            view = jnp.stack([real[:, half], imag[:, half]], axis=1)
            return view.reshape(width, rhs).astype(jnp.bfloat16)

        real, imag = fine[:, 0], fine[:, 1]
        right = jnp.concatenate(
            [ordered(real, imag, 0), ordered(real, imag, 1),
             ordered(imag, -real, 0), ordered(imag, -real, 1)], axis=1
        )
        total = jnp.dot(weights, right, preferred_element_type=jnp.float32)
        return jnp.concatenate(
            [
                total[:null, :rhs], total[null:, rhs : 2 * rhs],
                total[:null, 2 * rhs : 3 * rhs], total[null:, 3 * rhs :],
            ],
            axis=0,
        )

    def part_copy(slot):
        return pltpu.make_async_remote_copy(
            src_ref=part_out.at[slot], dst_ref=part_in.at[slot],
            send_sem=psend.at[slot], recv_sem=precv.at[slot],
            device_id={"ta": partner}, device_id_type=MESH,
        )

    def source_copy(slot, origin):
        return pltpu.make_async_remote_copy(
            src_ref=sum_out.at[slot], dst_ref=source_ref.at[origin],
            send_sem=ssend.at[slot], recv_sem=srecv.at[origin],
            device_id={"ta": flipped(chip, slot, bits - 1) * 2 + core}, device_id_type=MESH,
        )

    def pair(step):
        other = flipped(chip, step, bits - 1)
        away = other * 2 + 1 - core
        weights_copy(me, partner, away).wait_recv()
        part_out[step] = restricted(away, weights_in[away])
        part_copy(step).start()
        kept = other * 2 + core
        weights_copy(me, partner, kept).wait_recv()
        part_keep[step] = restricted(kept, weights_in[kept])

    def finish(step):
        part_copy(step).wait_recv()
        sum_out[step] = part_keep[step] + part_in[step]
        source_copy(step, chip).start()

    weights_copy(me, partner, partner).wait_recv()
    part_out[0] = restricted(partner, weights_in[partner])
    part_copy(0).start()
    part_keep[0] = restricted(me, weights_ref[me])
    pair(1)
    part_copy(0).wait_recv()
    source_ref[chip] = part_keep[0] + part_in[0]

    def pair_step(step, carry):
        pair(step)
        finish(step - 1)
        return carry

    lax.fori_loop(2, chips, pair_step, 0)
    finish(chips - 1)

    def source_wait(step, carry):
        source_copy(step, flipped(chip, step, bits - 1)).wait_recv()
        return carry

    lax.fori_loop(1, chips, source_wait, 0)

    mass = mass_ref[0]
    base = (me // LZ) * LZ
    z_at = me % LZ
    above = base + (z_at + 1) % LZ
    below = base + (z_at + LZ - 1) % LZ
    other_time = (me + LZ) % count
    targets = (other_time, above, below)
    lines = sites // LX

    def place(site, dx, dy):
        return ((site // LX + dy) % lines) * LX + (site % LX + dx) % LX

    def halo_copy(iteration, which):
        return pltpu.make_async_remote_copy(
            src_ref=round_ref.at[iteration], dst_ref=halo_ref.at[iteration, which],
            send_sem=hsend.at[iteration, which], recv_sem=hrecv.at[iteration, which],
            device_id={"ta": targets[which]}, device_id_type=MESH,
        )

    def stat_copy(iteration, other, origin):
        return pltpu.make_async_remote_copy(
            src_ref=stat_out.at[iteration], dst_ref=stat_in.at[iteration, origin],
            send_sem=gsend.at[iteration, other], recv_sem=grecv.at[iteration, origin],
            device_id={"ta": other}, device_id_type=MESH,
        )

    def times(factor, value):
        real, imag = value[:comps], value[comps:]
        return jnp.concatenate(
            [factor[0] * real - factor[1] * imag, factor[0] * imag + factor[1] * real], axis=0
        )

    factors, alphas, epsilons, overlap = [], [], [], None
    backs = []
    for it in range(ITERS):
        old = source_ref if it == 0 else res_ref
        for site in range(sites):
            round_ref[it, site] = old[site].astype(jnp.bfloat16)
        for which in range(3):
            halo_copy(it, which).start()
        for site in range(sites):
            wide_ref[site] = widened(round_ref[it, site])
        for site in range(sites):
            steps = ((0, 0), (1, 0), (-1, 0), (0, 1), (0, -1))
            right = jnp.concatenate([wide_ref[place(site, dx, dy)] for dx, dy in steps], axis=0)
            acc_ref[site] = jnp.dot(near_ref[site], right, preferred_element_type=jnp.float32)
        halo_copy(it, 2).wait_recv()
        halo_copy(it, 1).wait_recv()
        for site in range(sites):
            right = jnp.concatenate(
                [widened(halo_ref[it, 2, site]), widened(halo_ref[it, 1, site])], axis=0
            )
            acc_ref[site] += jnp.dot(zlinks_ref[site], right, preferred_element_type=jnp.float32)
        halo_copy(it, 0).wait_recv()
        sums = [0.0] * (3 + 2 * it)
        for site in range(sites):
            wide = widened(halo_ref[it, 0, site])
            right = jnp.concatenate([wide, wide], axis=0)
            product = acc_ref[site] + jnp.dot(
                tlinks_ref[site], right, preferred_element_type=jnp.float32
            )
            rounded = mass * round_ref[it, site].astype(jnp.float32)
            q_re = product[:, :rhs] + rounded[:comps]
            q_im = product[:, rhs:] + rounded[comps:]
            acc_ref[site] = jnp.concatenate([q_re, q_im], axis=1)
            r_re, r_im = old[site, :comps], old[site, comps:]
            sums[0] += q_re * q_re + q_im * q_im
            sums[1] += q_re * r_re + q_im * r_im
            sums[2] += q_re * r_im - q_im * r_re
            for j in range(it):
                b_re, b_im = basis_q[j, site, :comps], basis_q[j, site, comps:]
                sums[3 + 2 * j] += b_re * q_re + b_im * q_im
                sums[4 + 2 * j] += b_re * q_im - b_im * q_re
        lines_of = [jnp.sum(value, axis=0, keepdims=True) for value in sums]
        lines_of += [jnp.zeros((8 - len(lines_of), rhs), jnp.float32)]
        stats = jnp.concatenate(lines_of, axis=0)
        stat_out[it] = stats

        def send_stats(step, carry, it=it):
            other = flipped(me, count - 1 - step, bits)
            stat_copy(it, other, me).start()
            return carry

        lax.fori_loop(0, count - 1, send_stats, 0)
        stat_in[it, me] = stats

        def wait_stats(step, carry, it=it):
            other = flipped(me, step, bits)
            stat_copy(it, other, other).wait_recv()
            return carry

        lax.fori_loop(1, count, wait_stats, 0)
        total = jnp.sum(stat_in[it], axis=0)
        squared, cross_re, cross_im = total[0:1], total[1:2], total[2:3]
        coefs = [(total[3 + 2 * j : 4 + 2 * j], total[4 + 2 * j : 5 + 2 * j]) for j in range(it)]
        for j, (c_re, c_im) in enumerate(coefs):
            squared = squared - (c_re * c_re + c_im * c_im) * (1.0 + epsilons[j])
            cross_re = cross_re - (c_re * backs[j][0] + c_im * backs[j][1])
            cross_im = cross_im - (c_re * backs[j][1] - c_im * backs[j][0])
        if it == 2:
            (a_re, a_im), (b_re, b_im) = coefs
            pair_re, pair_im = a_re * b_re + a_im * b_im, a_re * b_im - a_im * b_re
            squared = squared + 2.0 * (pair_re * overlap[0] - pair_im * overlap[1])
        factor = 1.0 / jnp.sqrt(squared + 1e-06)
        alpha = (cross_re * factor, cross_im * factor)
        epsilon = 1e-06 * factor * factor
        if it == 1:
            overlap = (coefs[0][0] * epsilons[0] * factor, coefs[0][1] * epsilons[0] * factor)
            backs[0] = (
                backs[0][0] - (alpha[0] * overlap[0] - alpha[1] * overlap[1]),
                backs[0][1] - (alpha[0] * overlap[1] + alpha[1] * overlap[0]),
            )
        backs.append((alpha[0] * epsilon, alpha[1] * epsilon))
        epsilons.append(epsilon)
        for site in range(sites):
            residual = old[site]
            q = acc_ref[site]
            q = jnp.concatenate([q[:, :rhs], q[:, rhs:]], axis=0)
            p = residual
            for j in range(it):
                q = q - times(coefs[j], basis_q[j, site])
                p = p - times(coefs[j], basis_p[j, site])
            q = q * factor
            p = p * factor
            if it < ITERS - 1:
                basis_q[it, site] = q
                basis_p[it, site] = p
            step = times(alpha, p)
            sol_ref[site] = step if it == 0 else sol_ref[site] + step
            res_ref[site] = residual - times(alpha, q)

    def drain(step, carry):
        other = flipped(me, step, bits)
        weights_copy(other, other, me).wait_send()
        for it in range(ITERS):
            stat_copy(it, other, me).wait_send()
        return carry

    lax.fori_loop(1, count, drain, 0)
    part_copy(0).wait_send()

    def drain_parts(step, carry):
        part_copy(step).wait_send()
        source_copy(step, chip).wait_send()
        return carry

    lax.fori_loop(1, chips, drain_parts, 0)
    for it in range(ITERS):
        for which in range(3):
            halo_copy(it, which).wait_send()


def shards_kernel(fine_source, projectors, stencil_links, quark_mass):
    count = lax.axis_size("ta")
    planes, local_columns, _, _, null, rhs = fine_source.shape
    sites, comps = stencil_links.shape[1], stencil_links.shape[2]
    rows = local_columns * 4 * null
    fine = fine_source.reshape(planes, rows, rhs)
    proj = projectors.reshape(count, local_columns, 4 * null * null)
    width = local_columns * comps
    links = stencil_links.reshape(sites, comps, 18 * comps)
    chips = count // 2
    vector = (sites, 2 * comps, rhs)
    f32, bf16 = jnp.float32, jnp.bfloat16
    dma = pltpu.SemaphoreType.DMA
    vmem = pl.BlockSpec(memory_space=pltpu.VMEM)
    hbm = pl.BlockSpec(memory_space=pl.ANY)
    parts = (chips, 2 * comps, rhs)
    sol, res = pl.pallas_call(
        functools.partial(solve_kernel, count, sites, comps),
        out_shape=[jax.ShapeDtypeStruct(vector, f32)] * 2,
        in_specs=[pl.BlockSpec(memory_space=pltpu.SMEM), vmem, hbm, hbm],
        out_specs=[vmem, vmem],
        scratch_shapes=[
            pltpu.VMEM(fine.shape, bf16),
            pltpu.VMEM(links.shape, bf16),
            pltpu.VMEM((sites, comps, 10 * comps), bf16),
            pltpu.VMEM((sites, comps, 4 * comps), bf16),
            pltpu.VMEM((sites, comps, 4 * comps), bf16),
            pltpu.VMEM((width, width), bf16),
            pltpu.VMEM((count, comps, width), bf16),
            pltpu.VMEM((count, comps, width), bf16),
            pltpu.VMEM(parts, f32),
            pltpu.VMEM(parts, f32),
            pltpu.VMEM(parts, f32),
            pltpu.VMEM(parts, f32),
            pltpu.VMEM(vector, f32),
            pltpu.VMEM((sites, 2 * comps, 2 * rhs), bf16),
            pltpu.VMEM((ITERS, *vector), bf16),
            pltpu.VMEM((ITERS, 3, *vector), bf16),
            pltpu.VMEM((sites, comps, 2 * rhs), f32),
            pltpu.VMEM((ITERS - 1, *vector), f32),
            pltpu.VMEM((ITERS - 1, *vector), f32),
            pltpu.VMEM((ITERS, 8, rhs), f32),
            pltpu.VMEM((ITERS, count, 8, rhs), f32),
            dma((2,)),
            dma((count,)),
            dma((count,)),
            dma((chips,)),
            dma((chips,)),
            dma((chips,)),
            dma((chips,)),
            dma((ITERS, 3)),
            dma((ITERS, 3)),
            dma((ITERS, count)),
            dma((ITERS, count)),
        ],
        compiler_params=pltpu.CompilerParams(
            collective_id=0, has_side_effects=True, vmem_limit_bytes=60 * 1024 * 1024
        ),
    )(quark_mass, proj, fine, links)
    return sol.reshape(1, *vector), res.reshape(1, *vector)


def shards(fine_source, projectors, stencil_links, quark_mass):
    count = lax.axis_size("ta")
    sites = stencil_links.shape[1]
    local_columns = fine_source.shape[1]
    block = projectors.shape[1] // sites
    fits = (
        count == 2 * LZ
        and count == 2 * sites
        and count & (count - 1) == 0
        and block == 2 * local_columns
        and stencil_links.shape[2] % local_columns == 0
        and fine_source.shape[0] == count
        and ITERS == 3
    )
    chosen = shards_kernel if fits else shards_general
    return chosen(fine_source, projectors, stencil_links, quark_mass)


def solution(mesh):
    return jax.shard_map(
        shards,
        mesh=mesh,
        in_specs=(
            P("cfg", "ta", None, None, None, None),
            P(("cfg", "ta"), None, None),
            P(("cfg", "ta"), None, None, None),
            P("cfg"),
        ),
        out_specs=(P(("cfg", "ta"), None, None, None), P(("cfg", "ta"), None, None, None)),
        check_vma=False,
    )
```

```python
import functools
import math

import jax
import jax.numpy as jnp
from jax import lax
from jax.experimental import pallas as pl
from jax.experimental.pallas import tpu as pltpu
from jax.sharding import PartitionSpec as P

LX = 4
LZ = 8
ITERS = 3


def from_behind(value, axis, steps):
    count = lax.axis_size(axis)
    pairs = [(source, (source + steps) % count) for source in range(count)]
    return lax.ppermute(value, axis, pairs)


def real_weights(proj_view):
    proj_re = proj_view[..., 0, :]
    proj_im = proj_view[..., 1, :]
    first_row = jnp.stack([proj_re, proj_im], axis=-4)
    second_row = jnp.stack([-proj_im, proj_re], axis=-4)
    return jnp.stack([first_row, second_row], axis=-5)


def inner_local(left, right, comp_count):
    left_re = left[:, :comp_count]
    left_im = left[:, comp_count:]
    right_re = right[:, :comp_count]
    right_im = right[:, comp_count:]
    return (
        jnp.sum(left_re * right_re + left_im * right_im, axis=(0, 1)),
        jnp.sum(left_re * right_im - left_im * right_re, axis=(0, 1)),
    )


def scaled(vector, factor_re, factor_im, comp_count):
    vector_re = vector[:, :comp_count]
    vector_im = vector[:, comp_count:]
    return jnp.concatenate(
        [
            factor_re * vector_re - factor_im * vector_im,
            factor_re * vector_im + factor_im * vector_re,
        ],
        axis=1,
    )


def shards_general(fine_source, projectors, stencil_links, quark_mass):
    comp_count = stencil_links.shape[2]
    null_count = comp_count // 2
    site_count = stencil_links.shape[1]
    column_count = projectors.shape[1]
    block_count = column_count // site_count
    fine_count = fine_source.shape[4]
    rhs_count = fine_source.shape[5]
    plane_count = fine_source.shape[0]
    moved_proj = lax.all_to_all(projectors, "ta", split_axis=1, concat_axis=0, tiled=True)
    local_columns = fine_source.shape[1]
    group_size = math.gcd(block_count, local_columns)
    groups = local_columns // group_size
    weights = real_weights(
        moved_proj.reshape(plane_count, groups, group_size, 2, null_count, 2, fine_count)
    )
    fine_local = fine_source.reshape(plane_count, groups, group_size, 2, 2, fine_count, rhs_count)
    partial_sums = jnp.einsum(
        "pmgdchvk,pmgchkr->pmdhvr", weights, fine_local, preferred_element_type=jnp.float32
    )
    partial_sums = partial_sums.reshape(plane_count, groups, 2 * comp_count, rhs_count)
    collected = lax.all_to_all(partial_sums, "ta", split_axis=0, concat_axis=1, tiled=True)
    source = jnp.sum(
        collected.reshape(site_count, block_count // group_size, 2 * comp_count, rhs_count), axis=1
    )
    link_view = stencil_links.reshape(site_count, comp_count, 9, 2, comp_count)
    link_re = link_view[:, :, :, 0, :]
    link_im = link_view[:, :, :, 1, :]
    upper_rows = jnp.stack([link_re, -link_im], axis=3)
    lower_rows = jnp.stack([link_im, link_re], axis=3)
    real_operator = jnp.stack([upper_rows, lower_rows], axis=1).reshape(
        site_count, 2 * comp_count, 18 * comp_count
    )
    mass_value = quark_mass[0]
    z_position = lax.axis_index("ta") % LZ
    line_count = site_count // LX

    def flatten_sites(shifted):
        return shifted.reshape(site_count, 2 * comp_count, rhs_count)

    solution = jnp.zeros_like(source)
    residual = source
    basis_q = []
    basis_p = []
    for iteration in range(ITERS):
        direction = residual
        rounded = residual.astype(jnp.bfloat16)
        plane_view = rounded.reshape(line_count, LX, 2 * comp_count, rhs_count)
        x_plus = flatten_sites(jnp.roll(plane_view, -1, axis=1))
        x_minus = flatten_sites(jnp.roll(plane_view, 1, axis=1))
        y_plus = flatten_sites(jnp.roll(plane_view, -1, axis=0))
        y_minus = flatten_sites(jnp.roll(plane_view, 1, axis=0))
        z_plus_near = from_behind(rounded, "ta", -1)
        z_minus_near = from_behind(rounded, "ta", 1)
        upper_pair = from_behind(jnp.stack([rounded, z_minus_near], axis=0), "ta", -LZ)
        lower_pair = from_behind(jnp.stack([rounded, z_plus_near], axis=0), "ta", LZ)
        t_plus = upper_pair[0]
        t_minus = lower_pair[0]
        z_plus = jnp.where(z_position == LZ - 1, lower_pair[1], z_plus_near)
        z_minus = jnp.where(z_position == 0, upper_pair[1], z_minus_near)
        stacked = jnp.stack(
            [rounded, x_plus, x_minus, y_plus, y_minus, z_plus, z_minus, t_plus, t_minus], axis=1
        )
        stacked = stacked.reshape(site_count, 18 * comp_count, rhs_count)
        product = jnp.einsum(
            "sij,sjr->sir", real_operator, stacked, preferred_element_type=jnp.float32
        )
        mapped = product + mass_value * rounded.astype(jnp.float32)
        square_loc = inner_local(mapped, mapped, comp_count)[0]
        cross_re, cross_im = inner_local(mapped, residual, comp_count)
        if iteration > 0:
            coef_pairs = [inner_local(earlier, mapped, comp_count) for earlier in basis_q]
            back_pairs = [inner_local(earlier, residual, comp_count) for earlier in basis_q]
            coef_re = jnp.stack([pair[0] for pair in coef_pairs])
            coef_im = jnp.stack([pair[1] for pair in coef_pairs])
            back_re = jnp.stack([pair[0] for pair in back_pairs])
            back_im = jnp.stack([pair[1] for pair in back_pairs])
        else:
            coef_re = jnp.zeros((1, rhs_count), jnp.float32)
            coef_im = jnp.zeros((1, rhs_count), jnp.float32)
            back_re = jnp.zeros((1, rhs_count), jnp.float32)
            back_im = jnp.zeros((1, rhs_count), jnp.float32)
        square_all, cross_re, cross_im, coef_re, coef_im, back_re, back_im = lax.psum(
            (square_loc, cross_re, cross_im, coef_re, coef_im, back_re, back_im), "ta"
        )
        squared = square_all
        proj_re = cross_re
        proj_im = cross_im
        for number in range(iteration):
            mapped = mapped - scaled(basis_q[number], coef_re[number], coef_im[number], comp_count)
            direction = direction - scaled(
                basis_p[number], coef_re[number], coef_im[number], comp_count
            )
            squared = squared - (
                coef_re[number] * coef_re[number] + coef_im[number] * coef_im[number]
            )
            proj_re = proj_re - (
                coef_re[number] * back_re[number] + coef_im[number] * back_im[number]
            )
            proj_im = proj_im - (
                coef_re[number] * back_im[number] - coef_im[number] * back_re[number]
            )
        factor = 1.0 / jnp.sqrt(squared + 1e-06)
        unit_q = mapped * factor
        unit_p = direction * factor
        alpha_re = proj_re * factor
        alpha_im = proj_im * factor
        solution = solution + scaled(unit_p, alpha_re, alpha_im, comp_count)
        residual = residual - scaled(unit_q, alpha_re, alpha_im, comp_count)
        basis_q.append(unit_q)
        basis_p.append(unit_p)
    return (
        solution.reshape(1, site_count, 2 * comp_count, rhs_count),
        residual.reshape(1, site_count, 2 * comp_count, rhs_count),
    )


MESH = pl.DeviceIdType.MESH


def flipped(number, mask, bits):
    total = 0
    for bit in range(bits):
        size = 1 << bit
        total = total + (((number // size) % 2 + (mask // size) % 2) % 2) * size
    return total


def swapped(value):
    return pltpu.roll(value, value.shape[-1] // 2, value.ndim - 1)


def lower_lanes(shape):
    return lax.broadcasted_iota(jnp.int32, shape, len(shape) - 1) < shape[-1] // 2


def turned(value):
    other = swapped(value)
    return jnp.where(lower_lanes(value.shape), -other, other)


def widened(rounded):
    return jnp.concatenate(
        [rounded, turned(rounded.astype(jnp.float32)).astype(jnp.bfloat16)], axis=0
    )


def times(factor, value):
    return factor[0] * value + factor[1] * turned(value)


def solve_kernel(
    count, sites, comps,
    mass_ref, proj_ref, fine_hbm, links_hbm,
    sol_ref, res_ref,
    fine_ref, links_ref, near_ref, zlinks_ref, tlinks_ref, fold_ref,
    weights_ref, weights_in, part_keep, part_out, part_in, sum_out, source_ref,
    wide_ref, round_ref, halo_ref, acc_ref, sol_half, res_half, basis_q, basis_p, stat_out, stat_in,
    local_sem, wsend, wrecv, psend, precv, ssend, srecv, hsend, hrecv, gsend, grecv,
):
    me = lax.axis_index("ta")
    bits = count.bit_length() - 1
    core = me % 2
    chip = me // 2
    partner = chip * 2 + 1 - core
    chips = count // 2
    turns = [(1 - 2 * ((me // (1 << bit)) % 2)) * (1 << bit) for bit in range(bits)]
    others = [me]
    for step in range(1, count):
        top = step.bit_length() - 1
        others.append(others[step - (1 << top)] + turns[top])
    null = comps // 2
    rows = fine_ref.shape[1]
    rhs = fine_ref.shape[2]

    fine_copy = pltpu.make_async_copy(fine_hbm, fine_ref, local_sem.at[0])
    fine_copy.start()
    links_copy = pltpu.make_async_copy(links_hbm, links_ref, local_sem.at[1])
    links_copy.start()

    barrier = pltpu.get_barrier_semaphore()

    for other in others[1:]:
        pl.semaphore_signal(barrier, inc=1, device_id={"ta": other}, device_id_type=MESH)
    pl.semaphore_wait(barrier, count - 1)

    def weights_copy(slot, other, origin):
        return pltpu.make_async_remote_copy(
            src_ref=weights_ref.at[slot], dst_ref=weights_in.at[origin],
            send_sem=wsend.at[slot], recv_sem=wrecv.at[origin],
            device_id={"ta": other}, device_id_type=MESH,
        )

    columns = proj_ref.shape[1]
    width = columns * comps
    groups = comps // columns
    lane_at = lax.broadcasted_iota(jnp.int32, (columns, width), 1) // comps
    row_at = lax.broadcasted_iota(jnp.int32, (columns, width), 0)
    picks = (lane_at == row_at).astype(jnp.float32)
    fold_row = lax.broadcasted_iota(jnp.int32, (width, width), 0) % comps
    fold_lane = lax.broadcasted_iota(jnp.int32, (width, width), 1) % comps
    fold_ref[...] = (fold_row == fold_lane).astype(jnp.float32).astype(jnp.bfloat16)

    def arrange(slot):
        raw = proj_ref[slot].astype(jnp.float32)
        pieces = []
        for column in range(columns):
            for group in range(groups):
                row = raw[column : column + 1, group * width : (group + 1) * width]
                pieces.append(row * picks)
        left = jnp.concatenate(pieces, axis=0).astype(jnp.bfloat16)
        spread = jnp.dot(left, fold_ref[...], preferred_element_type=jnp.float32)
        total = spread[:comps] * picks[0:1]
        for column in range(1, columns):
            block = spread[column * comps : (column + 1) * comps]
            total = total + block * picks[column : column + 1]
        weights_ref[slot] = total.astype(jnp.bfloat16)

    def send_weights(step, carry):
        other = flipped(me, count - 1 - step, bits)
        arrange(other)
        weights_copy(other, other, me).start()
        return carry

    lax.fori_loop(0, count - 1, send_weights, 0)
    arrange(me)

    links_copy.wait()
    for site in range(sites):
        near_ref[site] = links_ref[site, :, : 10 * comps]
        zlinks_ref[site] = links_ref[site, :, 10 * comps : 14 * comps]
        tlinks_ref[site] = links_ref[site, :, 14 * comps : 18 * comps]
    fine_copy.wait()

    def restricted(plane, weights):
        fine = fine_ref[plane].astype(jnp.float32).reshape(columns, 2, 2, null, rhs)

        def ordered(real, imag, half):
            view = jnp.stack([real[:, half], imag[:, half]], axis=1)
            return view.reshape(width, rhs).astype(jnp.bfloat16)

        real, imag = fine[:, 0], fine[:, 1]
        right = jnp.concatenate(
            [ordered(real, imag, 0), ordered(real, imag, 1),
             ordered(imag, -real, 0), ordered(imag, -real, 1)], axis=1
        )
        total = jnp.dot(weights, right, preferred_element_type=jnp.float32)
        real = jnp.concatenate([total[:null, :rhs], total[null:, rhs : 2 * rhs]], axis=0)
        imag = jnp.concatenate(
            [total[:null, 2 * rhs : 3 * rhs], total[null:, 3 * rhs :]], axis=0
        )
        low = lower_lanes(real.shape)
        return jnp.stack(
            [jnp.where(low, real, swapped(imag)), jnp.where(low, swapped(real), imag)], axis=0
        )

    def part_copy(slot):
        return pltpu.make_async_remote_copy(
            src_ref=part_out.at[slot], dst_ref=part_in.at[slot],
            send_sem=psend.at[slot], recv_sem=precv.at[slot],
            device_id={"ta": partner}, device_id_type=MESH,
        )

    def source_copy(slot, origin):
        return pltpu.make_async_remote_copy(
            src_ref=sum_out.at[slot], dst_ref=source_ref.at[origin],
            send_sem=ssend.at[slot], recv_sem=srecv.at[origin],
            device_id={"ta": flipped(chip, slot, bits - 1) * 2 + core}, device_id_type=MESH,
        )

    def pair(step):
        other = flipped(chip, step, bits - 1)
        away = other * 2 + 1 - core
        weights_copy(me, partner, away).wait_recv()
        part_out[step] = restricted(away, weights_in[away])
        part_copy(step).start()
        kept = other * 2 + core
        weights_copy(me, partner, kept).wait_recv()
        part_keep[step] = restricted(kept, weights_in[kept])

    def finish(step):
        part_copy(step).wait_recv()
        sum_out[step] = part_keep[step] + part_in[step]
        source_copy(step, chip).start()

    weights_copy(me, partner, partner).wait_recv()
    part_out[0] = restricted(partner, weights_in[partner])
    part_copy(0).start()
    part_keep[0] = restricted(me, weights_ref[me])
    pair(1)
    part_copy(0).wait_recv()
    source_ref[chip] = part_keep[0] + part_in[0]

    def pair_step(step, carry):
        pair(step)
        finish(step - 1)
        return carry

    lax.fori_loop(2, chips, pair_step, 0)
    finish(chips - 1)

    for step in range(1, chips):
        source_copy(step, others[2 * step] // 2).wait_recv()

    mass = mass_ref[0]
    base = (me // LZ) * LZ
    z_at = me % LZ
    above = base + (z_at + 1) % LZ
    below = base + (z_at + LZ - 1) % LZ
    other_time = (me + LZ) % count
    targets = (other_time, above, below)
    lines = sites // LX

    def place(site, dx, dy):
        return ((site // LX + dy) % lines) * LX + (site % LX + dx) % LX

    def halo_copy(it, half, which):
        return pltpu.make_async_remote_copy(
            src_ref=round_ref.at[it, half], dst_ref=halo_ref.at[it, half, which],
            send_sem=hsend.at[it, half, which], recv_sem=hrecv.at[it, half, which],
            device_id={"ta": targets[which]}, device_id_type=MESH,
        )

    def stat_copy(it, half, other, origin):
        return pltpu.make_async_remote_copy(
            src_ref=stat_out.at[it, half], dst_ref=stat_in.at[it, half, origin],
            send_sem=gsend.at[it, half, other], recv_sem=grecv.at[it, half, origin],
            device_id={"ta": other}, device_id_type=MESH,
        )

    def residual_at(it, half, site):
        return source_ref[site, half] if it == 0 else res_half[half, site]

    def send_halo(it, half):
        for site in range(sites):
            round_ref[it, half, site] = residual_at(it, half, site).astype(jnp.bfloat16)
        for which in range(3):
            halo_copy(it, half, which).start()

    def near_product(it, half):
        for site in range(sites):
            wide_ref[half, site] = widened(round_ref[it, half, site])
        steps = ((0, 0), (1, 0), (-1, 0), (0, 1), (0, -1))
        for site in range(sites):
            right = jnp.concatenate(
                [wide_ref[half, place(site, dx, dy)] for dx, dy in steps], axis=0
            )
            acc_ref[half, site] = jnp.dot(
                near_ref[site], right, preferred_element_type=jnp.float32
            )

    def far_product(it, half):
        halo_copy(it, half, 2).wait_recv()
        halo_copy(it, half, 1).wait_recv()
        for site in range(sites):
            right = jnp.concatenate(
                [widened(halo_ref[it, half, 2, site]), widened(halo_ref[it, half, 1, site])],
                axis=0,
            )
            acc_ref[half, site] += jnp.dot(
                zlinks_ref[site], right, preferred_element_type=jnp.float32
            )
        halo_copy(it, half, 0).wait_recv()
        sums = [0.0] * (3 + 2 * it)
        for site in range(sites):
            wide = widened(halo_ref[it, half, 0, site])
            right = jnp.concatenate([wide, wide], axis=0)
            product = acc_ref[half, site] + jnp.dot(
                tlinks_ref[site], right, preferred_element_type=jnp.float32
            )
            q = product + mass * round_ref[it, half, site].astype(jnp.float32)
            acc_ref[half, site] = q
            r = residual_at(it, half, site)
            q_other = swapped(q)
            sums[0] += q * q
            sums[1] += q * r
            sums[2] += q * swapped(r)
            for j in range(it):
                b = basis_q[j, half, site]
                sums[3 + 2 * j] += b * q
                sums[4 + 2 * j] += b * q_other
        lines_of = [jnp.sum(value, axis=0, keepdims=True) for value in sums]
        lines_of += [jnp.zeros((8 - len(lines_of), rhs), jnp.float32)]
        stats = jnp.concatenate(lines_of, axis=0)
        stat_out[it, half] = stats

        for other in others[:0:-1]:
            stat_copy(it, half, other, me).start()
        stat_in[it, half, me] = stats

    scalars = [([], [], [], []) for _ in range(2)]

    def update(it, half):
        for other in others[1:]:
            stat_copy(it, half, other, other).wait_recv()
        total = jnp.sum(stat_in[it, half], axis=0)
        moved = swapped(total)
        reals = total + moved
        imags = jnp.where(lower_lanes(total.shape), total - moved, moved - total)
        backs, epsilons, overlaps, _ = scalars[half]
        squared, cross_re, cross_im = reals[0:1], reals[1:2], imags[2:3]
        coefs = [
            (reals[3 + 2 * j : 4 + 2 * j], imags[4 + 2 * j : 5 + 2 * j]) for j in range(it)
        ]
        for j, (c_re, c_im) in enumerate(coefs):
            squared = squared - (c_re * c_re + c_im * c_im) * (1.0 + epsilons[j])
            cross_re = cross_re - (c_re * backs[j][0] + c_im * backs[j][1])
            cross_im = cross_im - (c_re * backs[j][1] - c_im * backs[j][0])
        if it == 2:
            (a_re, a_im), (b_re, b_im) = coefs
            pair_re, pair_im = a_re * b_re + a_im * b_im, a_re * b_im - a_im * b_re
            squared = squared + 2.0 * (pair_re * overlaps[0][0] - pair_im * overlaps[0][1])
        factor = 1.0 / jnp.sqrt(squared + 1e-06)
        alpha = (cross_re * factor, cross_im * factor)
        epsilon = 1e-06 * factor * factor
        if it == 1:
            over = (coefs[0][0] * epsilons[0] * factor, coefs[0][1] * epsilons[0] * factor)
            overlaps.append(over)
            backs[0] = (
                backs[0][0] - (alpha[0] * over[0] - alpha[1] * over[1]),
                backs[0][1] - (alpha[0] * over[1] + alpha[1] * over[0]),
            )
        backs.append((alpha[0] * epsilon, alpha[1] * epsilon))
        epsilons.append(epsilon)
        for site in range(sites):
            residual = residual_at(it, half, site)
            q = acc_ref[half, site]
            p = residual
            for j in range(it):
                q = q - times(coefs[j], basis_q[j, half, site])
                p = p - times(coefs[j], basis_p[j, half, site])
            q = q * factor
            p = p * factor
            if it < ITERS - 1:
                basis_q[it, half, site] = q
                basis_p[it, half, site] = p
            step = times(alpha, p)
            sol_half[half, site] = step if it == 0 else sol_half[half, site] + step
            res_half[half, site] = residual - times(alpha, q)

    for half in range(2):
        send_halo(0, half)
    for half in range(2):
        near_product(0, half)
    for it in range(ITERS):
        for half in range(2):
            far_product(it, half)
        for half in range(2):
            update(it, half)
            if it < ITERS - 1:
                send_halo(it + 1, half)
                near_product(it + 1, half)
    for from_ref, to_ref in ((sol_half, sol_ref), (res_half, res_ref)):
        for site in range(sites):
            first, second = from_ref[0, site], from_ref[1, site]
            low = lower_lanes(first.shape)
            to_ref[site, :comps] = jnp.where(low, first, swapped(second))
            to_ref[site, comps:] = jnp.where(low, swapped(first), second)

    for other in others[1:]:
        weights_copy(other, other, me).wait_send()
        for it in range(ITERS):
            for half in range(2):
                stat_copy(it, half, other, me).wait_send()
    part_copy(0).wait_send()

    for step in range(1, chips):
        part_copy(step).wait_send()
        source_copy(step, chip).wait_send()
    for it in range(ITERS):
        for half in range(2):
            for which in range(3):
                halo_copy(it, half, which).wait_send()


def shards_kernel(fine_source, projectors, stencil_links, quark_mass):
    count = lax.axis_size("ta")
    planes, local_columns, _, _, null, rhs = fine_source.shape
    sites, comps = stencil_links.shape[1], stencil_links.shape[2]
    rows = local_columns * 4 * null
    fine = fine_source.reshape(planes, rows, rhs)
    proj = projectors.reshape(count, local_columns, 4 * null * null)
    width = local_columns * comps
    links = stencil_links.reshape(sites, comps, 18 * comps)
    chips = count // 2
    vector = (sites, 2 * comps, rhs)
    f32, bf16 = jnp.float32, jnp.bfloat16
    dma = pltpu.SemaphoreType.DMA
    vmem = pl.BlockSpec(memory_space=pltpu.VMEM)
    hbm = pl.BlockSpec(memory_space=pl.ANY)
    parts = (chips, 2, comps, rhs)
    half = (sites, comps, rhs)
    sol, res = pl.pallas_call(
        functools.partial(solve_kernel, count, sites, comps),
        out_shape=[jax.ShapeDtypeStruct(vector, f32)] * 2,
        in_specs=[pl.BlockSpec(memory_space=pltpu.SMEM), vmem, hbm, hbm],
        out_specs=[vmem, vmem],
        scratch_shapes=[
            pltpu.VMEM(fine.shape, bf16),
            pltpu.VMEM(links.shape, bf16),
            pltpu.VMEM((sites, comps, 10 * comps), bf16),
            pltpu.VMEM((sites, comps, 4 * comps), bf16),
            pltpu.VMEM((sites, comps, 4 * comps), bf16),
            pltpu.VMEM((width, width), bf16),
            pltpu.VMEM((count, comps, width), bf16),
            pltpu.VMEM((count, comps, width), bf16),
            pltpu.VMEM(parts, f32),
            pltpu.VMEM(parts, f32),
            pltpu.VMEM(parts, f32),
            pltpu.VMEM(parts, f32),
            pltpu.VMEM((sites, 2, comps, rhs), f32),
            pltpu.VMEM((2, sites, 2 * comps, rhs), bf16),
            pltpu.VMEM((ITERS, 2, *half), bf16),
            pltpu.VMEM((ITERS, 2, 3, *half), bf16),
            pltpu.VMEM((2, *half), f32),
            pltpu.VMEM((2, *half), f32),
            pltpu.VMEM((2, *half), f32),
            pltpu.VMEM((ITERS - 1, 2, *half), f32),
            pltpu.VMEM((ITERS - 1, 2, *half), f32),
            pltpu.VMEM((ITERS, 2, 8, rhs), f32),
            pltpu.VMEM((ITERS, 2, count, 8, rhs), f32),
            dma((2,)),
            dma((count,)),
            dma((count,)),
            dma((chips,)),
            dma((chips,)),
            dma((chips,)),
            dma((chips,)),
            dma((ITERS, 2, 3)),
            dma((ITERS, 2, 3)),
            dma((ITERS, 2, count)),
            dma((ITERS, 2, count)),
        ],
        compiler_params=pltpu.CompilerParams(
            collective_id=0, has_side_effects=True, vmem_limit_bytes=60 * 1024 * 1024
        ),
    )(quark_mass, proj, fine, links)
    return sol.reshape(1, *vector), res.reshape(1, *vector)


def shards(fine_source, projectors, stencil_links, quark_mass):
    count = lax.axis_size("ta")
    sites = stencil_links.shape[1]
    local_columns = fine_source.shape[1]
    block = projectors.shape[1] // sites
    fits = (
        count == 2 * LZ
        and count == 2 * sites
        and count & (count - 1) == 0
        and block == 2 * local_columns
        and stencil_links.shape[2] % local_columns == 0
        and fine_source.shape[0] == count
        and ITERS == 3
        and fine_source.shape[5] % 2 == 0
    )
    chosen = shards_kernel if fits else shards_general
    return chosen(fine_source, projectors, stencil_links, quark_mass)


def solution(mesh):
    return jax.shard_map(
        shards,
        mesh=mesh,
        in_specs=(
            P("cfg", "ta", None, None, None, None),
            P(("cfg", "ta"), None, None),
            P(("cfg", "ta"), None, None, None),
            P("cfg"),
        ),
        out_specs=(P(("cfg", "ta"), None, None, None), P(("cfg", "ta"), None, None, None)),
        check_vma=False,
    )
```
